32 devices in a mesh: space: 8 (over y, x, core), mode: 4 (over z).
Axes of the slice: x: 2, y: 2, z: 4, core: 2. Of those that a mesh axis runs over, the one named last changes fastest.
Arguments:
- occupation_deviation: float32 [2048, 16, 4, 128], P('mode', 'space'), may hold values from -6 to 6
- initial_thermal_offset: float32 [16, 4, 128], P('space'), may hold values from -6 to 6
- branch_specific_warmth: float32 [2048], replicated, may hold values from 0.2 to 2
- courant_numbers: float32 [3, 2048], P(None, 'mode'), may hold values from 0.02 to 0.3
- sign_quadrant: int32 [2048], P('mode'), may hold values from 0 to 7
- scattering_matrix: bfloat16 [2048, 2048], P('mode'), may hold values from -1 to 1
Outputs:
- population_out: float32 [2048, 16, 4, 128], P('mode', 'space')
- thermal_offset: float32 [16, 4, 128], P('space')
The draws below stay inside these ranges and needn't reach their ends.
All inputs are finite; a program needn't handle non-finite values.
Results may differ from the reference program's by a relative error of at most 0.002.
Values may be sent and summed in bfloat16 or wider, within the bound.
No kernel may reach another device: no remote copies, remote signals or barrier semaphores. Data moves between devices by JAX's collectives and lax.ppermute only.
A program may use at most 64 MiB of HBM per device.

```python
import math
import jax
import jax.numpy as jnp
from jax import lax

M = 2048
GRID_LENGTH_TWO = 4
GRID_LENGTH_THREE = 128
ITERS = 3
GRID_LENGTH_ONE = 16


def draw_scattering_matrix(key, part):
    key_diag, key_off = jax.random.split(jax.random.fold_in(key, 17))
    diag_values = jnp.exp(jax.random.uniform(key_diag, (M,), jnp.float32, jnp.log(0.3), jnp.log(0.8)))
    off_part = jax.random.normal(key_off, (M, M), jnp.float32) * (0.25 / jnp.sqrt(M * 1.0))
    return (off_part + jnp.diag(diag_values)).astype(jnp.bfloat16)


def touch_ends(array, stream_key, least, top_value):
    longest = array.shape.index(max(array.shape))
    spots = []
    for shift in (0, 1):
        where = [jax.random.randint(jax.random.fold_in(stream_key, axis), (), 0, length) for axis, length in enumerate(array.shape)]
        where[longest] = (where[longest] + shift) % array.shape[longest]
        spots.append(tuple(where))
    return array.at[spots[0]].set(least).at[spots[1]].set(top_value)


def levels(rng, extent, cuts, smallest, largest):
    loudness = 1.0
    for position, shards_of in cuts:
        steps = jax.random.uniform(jax.random.fold_in(jax.random.fold_in(rng, 6), position), (shards_of,), jnp.float32, smallest / len(cuts), largest / len(cuts))
        loudness = loudness * jnp.repeat(jnp.exp(steps), extent[position] // shards_of).reshape((-1,) + (1,) * (len(extent) - 1 - position))
    return loudness


def gaussian(stream_key, dims, spread, most, cuts=(), kind=jnp.bfloat16):
    array = spread * jax.random.normal(stream_key, dims, jnp.float32)
    if cuts:
        array = array * levels(stream_key, dims, cuts, -0.22, 0.18)
    return jnp.clip(array, -most, most).astype(kind)


def setup_inputs(seed: int = 0) -> dict:
    seeds = jax.random.split(jax.random.key(seed), 7)
    occupation_deviation = gaussian(seeds[0], (M, GRID_LENGTH_ONE, GRID_LENGTH_TWO, GRID_LENGTH_THREE), 1.0, 6.0, ((0, 4), (1, 8)), jnp.float32)
    initial_thermal_offset = gaussian(seeds[1], (GRID_LENGTH_ONE, GRID_LENGTH_TWO, GRID_LENGTH_THREE), 1.0, 6.0, ((0, 8),), jnp.float32)
    branch_specific_warmth = jnp.clip(jnp.exp(jax.random.uniform(seeds[2], (M,), jnp.float32, math.log(0.2), math.log(2.0))), 0.2, 2.0)
    courant_numbers = jnp.clip(jnp.exp(math.log(0.3) - 2.7080503 * jax.random.uniform(seeds[3], (3, M), jnp.float32) ** levels(seeds[3], (3, M), ((1, 4),), -0.2, 0.2)), 0.02, 0.3)
    sign_quadrant = touch_ends(jax.random.randint(seeds[4], (M,), 0, 8), jax.random.fold_in(seeds[4], 1), 0, 7).astype(jnp.int32)
    scattering_matrix = draw_scattering_matrix(jax.random.fold_in(seeds[6], 71), 0)
    return {"occupation_deviation": occupation_deviation, "initial_thermal_offset": initial_thermal_offset, "branch_specific_warmth": branch_specific_warmth, "courant_numbers": courant_numbers, "sign_quadrant": sign_quadrant, "scattering_matrix": scattering_matrix}


def advect(lattice_wave_carry, courant_numbers, sign_quadrant):
    advected = lattice_wave_carry
    for dim_index in range(3):
        grid_axis = dim_index + 1
        below_side = jnp.roll(lattice_wave_carry, 1, grid_axis)
        above_side = jnp.roll(lattice_wave_carry, -1, grid_axis)
        sign_bit = ((sign_quadrant >> dim_index) & 1).reshape(-1, 1, 1, 1)
        upwind = jnp.where(sign_bit == 1, above_side, below_side)
        advected = advected - courant_numbers[dim_index].reshape(-1, 1, 1, 1) * (lattice_wave_carry - upwind)
    return advected


def reference(occupation_deviation, initial_thermal_offset, branch_specific_warmth, courant_numbers, sign_quadrant, scattering_matrix):
    summed_specific_warmth = jnp.sum(branch_specific_warmth)
    lattice_wave_carry = occupation_deviation + branch_specific_warmth.reshape(-1, 1, 1, 1) * initial_thermal_offset[None]
    scattering_source = jnp.dot(scattering_matrix.astype(jnp.float32), branch_specific_warmth, precision=lax.Precision.HIGHEST)
    partition_extents = occupation_deviation.shape
    thermal_offset = jnp.zeros(partition_extents[1:], jnp.float32)
    for iteration in range(ITERS):
        upstream_occupation = advect(lattice_wave_carry, courant_numbers, sign_quadrant)
        moved_bf = upstream_occupation.astype(jnp.bfloat16)
        flat_rows = moved_bf.reshape(partition_extents[0], -1)
        internal_warmth_field = jnp.dot(branch_specific_warmth, flat_rows.astype(jnp.float32), precision=lax.Precision.HIGHEST)
        thermal_offset = (internal_warmth_field / summed_specific_warmth).reshape(partition_extents[1:])
        scattering_applied = jnp.dot(scattering_matrix, flat_rows, preferred_element_type=jnp.float32).reshape(partition_extents)
        lattice_wave_carry = upstream_occupation - scattering_applied + scattering_source.reshape(-1, 1, 1, 1) * thermal_offset[None]
    return lattice_wave_carry, thermal_offset
```

```python
import functools
import jax
import jax.numpy as jnp
from jax import lax
from jax.experimental import pallas as pl
from jax.experimental.pallas import tpu as pltpu
from jax.sharding import PartitionSpec as P

ITERS = 3
BOTH = ("space", "mode")
OCTAVES = 31
STEPS = 1024
F32 = jnp.float32
BF16 = jnp.bfloat16


def padded_2(cells, sides, width):
    for axis, dim in sides:
        count = lax.axis_size(axis)
        head = lax.slice_in_dim(cells, 0, width, axis=dim)
        tail = lax.slice_in_dim(cells, cells.shape[dim] - width, cells.shape[dim], axis=dim)
        cells = jnp.concatenate(
            [
                lax.ppermute(tail, axis, [(i, (i + 1) % count) for i in range(count)]),
                cells,
                lax.ppermute(head, axis, [((i + 1) % count, i) for i in range(count)]),
            ],
            axis=dim,
        )
    return cells


def advect(lattice_wave_carry, courant_numbers, sign_quadrant):
    padded = padded_2(lattice_wave_carry, (("space", 1),), 1)
    advected = lattice_wave_carry
    for dim_index in range(3):
        if dim_index == 0:
            below_side = padded[:, :-2]
            above_side = padded[:, 2:]
        else:
            below_side = jnp.roll(lattice_wave_carry, 1, dim_index + 1)
            above_side = jnp.roll(lattice_wave_carry, -1, dim_index + 1)
        sign_bit = (sign_quadrant >> dim_index & 1).reshape(-1, 1, 1, 1)
        upwind = jnp.where(sign_bit == 1, above_side, below_side)
        advected = advected - courant_numbers[dim_index].reshape(-1, 1, 1, 1) * (
            lattice_wave_carry - upwind
        )
    return advected


def plain_shards(occupation, offset, warmth, courant, quadrant, matrix):
    local_modes = occupation.shape[0]
    extents = occupation.shape
    cell_count = extents[1] * extents[2] * extents[3]
    first_mode = lax.axis_index("mode") * local_modes
    own_warmth = lax.dynamic_slice_in_dim(warmth, first_mode, local_modes)
    total_warmth = jnp.sum(warmth)
    state = occupation + own_warmth.reshape(-1, 1, 1, 1) * offset[None]
    relax = jnp.dot(matrix.astype(F32), warmth, precision=lax.Precision.HIGHEST)
    thermal = jnp.zeros(extents[1:], F32)
    for _ in range(ITERS):
        moved = advect(state, courant, quadrant)
        moved_bf = moved.astype(BF16)
        flat = lax.all_gather(moved_bf, "mode", axis=0, tiled=True).reshape(-1, cell_count)
        product = jnp.dot(matrix, flat, preferred_element_type=F32)
        energy = lax.psum(
            jnp.dot(
                own_warmth,
                moved_bf.reshape(local_modes, cell_count).astype(F32),
                precision=lax.Precision.HIGHEST,
            ),
            "mode",
        )
        thermal = (energy / total_warmth).reshape(extents[1:])
        state = moved - product.reshape(extents) + relax.reshape(-1, 1, 1, 1) * thermal[None]
    return state, thermal


def encode(x, inverse):
    y = jnp.maximum(jnp.abs(x) * inverse, 2.0**-OCTAVES)
    e = jnp.clip(jnp.floor(jnp.log2(y)), -float(OCTAVES), -1.0)
    v = (e + (OCTAVES - 1.0)) + y * jnp.exp2(-e)
    code = (v * STEPS + 0.5).astype(jnp.int32)
    return jnp.where(x < 0, -code, code).astype(jnp.int16)


def decode(code, scale):
    c = code.astype(jnp.int32)
    a = jnp.abs(c)
    e = (a >> 10) - OCTAVES
    f = (a & (STEPS - 1)).astype(F32) * (1.0 / STEPS) + 1.0
    v = f * jnp.exp2(e.astype(F32)) * scale
    return jnp.where(a == 0, 0.0, jnp.where(c < 0, -v, v))


def enter_kernel(order, modes, rows, depth, place, occ, offset, warmth, out, work):
    own = warmth[pl.ds(place[0], 1), :]
    for t in range(modes // 128):
        column = jnp.broadcast_to(own[:, t * 128 : t * 128 + 128], (depth, 128)).T
        for q in range(8):
            x = occ[pl.ds(t * 1024 + q, 128, stride=8), :]
            x = x + column * offset[pl.ds(q, 1), :]
            work[t, pl.ds(q, depth, stride=8), :] = x.T
        for k, device in enumerate(order):
            out[device, :, t * 128 : t * 128 + 128] = encode(
                work[t, k * rows : (k + 1) * rows, :], 2.0**-5
            )


def leave_kernel(order, modes, rows, depth, code, aux, out, work):
    cells = aux.shape[2] - 128
    for t in range(modes // 128):
        for k, device in enumerate(order):
            scale = aux[device, :, cells:]
            work[t, k * rows : (k + 1) * rows, :] = decode(
                code[device, :, t * 128 : t * 128 + 128], scale
            )
        for q in range(8):
            x = work[t, pl.ds(q, depth, stride=8), :]
            out[pl.ds(t * 1024 + q, 128, stride=8), :] = x.T


def iterate_kernel(first, last, dims, *refs):
    slices, ring, lane2, modes, blocks = dims
    cells = slices * ring
    width = modes // blocks
    refs = list(refs)
    source, low, high, courant, quadrant, warmth, matrix = refs[:7]
    refs = refs[7:]
    if not first:
        relax_in = refs.pop(0)
    if last:
        code_out, aux_out = refs[:2]
        refs = refs[2:]
    else:
        state_out, low_out, high_out = refs[:3]
        refs = refs[3:]
        if first:
            relax_out = refs.pop(0)
    moved_ref, left, panel, sems = refs[:4]
    state_ref = refs[4] if first else source

    copies = []
    for n in range(blocks):
        copy = pltpu.make_async_copy(
            matrix.at[pl.ds(n * width, width), :], panel.at[n], sems.at[n]
        )
        copy.start()
        copies.append(copy)

    if first:
        spaces = source.shape[0] // blocks
        for s in range(spaces):
            for n in range(blocks):
                x = decode(source[s * blocks + n], 2.0**5)
                for j in range(slices):
                    state_ref[j * ring + s * 8 : j * ring + s * 8 + 8, n * width : (n + 1) * width] = (
                        x[j * 8 : j * 8 + 8]
                    )

    step = 128
    row = lax.broadcasted_iota(jnp.int32, (ring, step), 0) % lane2
    energy = [jnp.zeros((ring, step), F32) for _ in range(slices)]
    largest = jnp.zeros((ring, step), F32)
    capacity = jnp.zeros((1, step), F32)
    for b in range(modes // step):
        at = slice(b * step, (b + 1) * step)
        c = [courant[d : d + 1, at] for d in range(3)]
        sign = quadrant[:, at]
        up = [jnp.broadcast_to((sign >> d & 1) == 1, (ring, step)) for d in range(3)]
        w = warmth[:, at]
        capacity = capacity + w
        x = [state_ref[j * ring : (j + 1) * ring, at] for j in range(slices)]
        if first:
            n, o = divmod(b * step, width)
            lo = jnp.concatenate(
                [low[s * blocks + n, :, o : o + step] for s in range(spaces)], axis=0
            )
            hi = jnp.concatenate(
                [high[s * blocks + n, :, o : o + step] for s in range(spaces)], axis=0
            )
            lo, hi = decode(lo, 2.0**5), decode(hi, 2.0**5)
        else:
            lo, hi = low[:, at].astype(F32), high[:, at].astype(F32)
        around = [lo] + x + [hi]
        for j in range(slices):
            y = x[j]
            below, above = pltpu.roll(y, lane2, 0), pltpu.roll(y, ring - lane2, 0)
            u0 = jnp.where(up[0], above, below)
            below = jnp.where(row == 0, pltpu.roll(y, ring - lane2 + 1, 0), pltpu.roll(y, 1, 0))
            above = jnp.where(
                row == lane2 - 1, pltpu.roll(y, lane2 - 1, 0), pltpu.roll(y, ring - 1, 0)
            )
            u1 = jnp.where(up[1], above, below)
            u2 = jnp.where(up[2], around[j + 2], around[j])
            moved = y - c[0] * (y - u0) - c[1] * (y - u1) - c[2] * (y - u2)
            bf = moved.astype(BF16)
            moved_ref[j * ring : (j + 1) * ring, at] = moved
            left[j * ring : (j + 1) * ring, at] = bf
            energy[j] = energy[j] + w * bf.astype(F32)
            if last:
                largest = jnp.maximum(largest, jnp.abs(moved))
    total = jnp.sum(capacity, axis=1, keepdims=True)
    thermal = jnp.concatenate(
        [jnp.sum(e, axis=1, keepdims=True) for e in energy], axis=0
    ) / total

    if first:
        w = warmth[...]
        w_high = w.astype(BF16)
        w_mid = (w - w_high.astype(F32)).astype(BF16)
        w_low = (w - w_high.astype(F32) - w_mid.astype(F32)).astype(BF16)
        pad = jnp.zeros((13, modes), F32)
        left[cells:, :] = jnp.concatenate(
            [w_high.astype(F32), w_mid.astype(F32), w_low.astype(F32), pad], axis=0
        ).astype(BF16)
    if last:
        peak = jnp.max(jnp.max(largest, axis=1, keepdims=True), axis=0, keepdims=True)
        peak = jnp.maximum(peak, 2.0**-100) * (4.0 * modes)
        flat = jnp.broadcast_to(thermal, (cells, 128)).T
        aux_out[:, :cells] = flat[0:1, :]
        aux_out[:, cells:] = jnp.broadcast_to(peak, (1, 128))
        inverse = 1.0 / peak

    for n in range(blocks):
        at = slice(n * width, (n + 1) * width)
        copies[n].wait()
        product = lax.dot_general(
            left[...], panel[n], (((1,), (1,)), ((), ())), preferred_element_type=F32
        )
        if first:
            relax = product[cells : cells + 1] + product[cells + 1 : cells + 2]
            relax = relax + product[cells + 2 : cells + 3]
            relax_out[:, at] = relax
        else:
            relax = relax_in[:, at]
        state = moved_ref[:, at] - product[:cells] + relax * thermal
        if last:
            for s in range(ring // 8):
                piece = jnp.concatenate(
                    [state[j * ring + s * 8 : j * ring + s * 8 + 8] for j in range(slices)], axis=0
                )
                code_out[s * blocks + n] = encode(piece, inverse)
        else:
            state_out[:, at] = state
            low_out[:, at] = state[:ring].astype(BF16)
            high_out[:, at] = state[cells - ring :].astype(BF16)


def vmem():
    return pl.BlockSpec(memory_space=pltpu.VMEM)


def ring_order(spaces, blocks):
    pairs = max(spaces // 2, 1)
    walk = [q ^ (q >> 1) for q in range(pairs)] if pairs & (pairs - 1) == 0 else list(range(pairs))
    order = []
    for c, q in enumerate(walk):
        for m in range(blocks) if c % 2 == 0 else reversed(range(blocks)):
            for s in range(q * spaces // pairs, (q + 1) * spaces // pairs):
                order.append(s * blocks + m)
    return order


def cell_shards(occupation, offset, warmth, courant, quadrant, matrix):
    spaces, blocks = lax.axis_size("space"), lax.axis_size("mode")
    width, planes, lane2, depth = occupation.shape
    modes = warmth.shape[0]
    slices = depth // (spaces * blocks)
    ring = spaces * planes * lane2
    cells = slices * ring
    rows = slices * 8
    order = ring_order(spaces, blocks)
    count = spaces * blocks
    forward = [(order[k], order[(k + 1) % count]) for k in range(count)]
    backward = [(b, a) for a, b in forward]

    part = width // spaces
    own = lax.dynamic_slice_in_dim(matrix, lax.axis_index("space") * part, part, axis=0)
    full = lax.all_gather(own, ("mode", "space"), axis=0, tiled=True)

    place = lax.axis_index("mode").astype(jnp.int32).reshape(1)
    grid_warmth = warmth.reshape(blocks, width)
    code = pl.pallas_call(
        functools.partial(enter_kernel, order, width, rows, depth),
        out_shape=jax.ShapeDtypeStruct((count, rows, width), jnp.int16),
        in_specs=[pl.BlockSpec(memory_space=pltpu.SMEM), vmem(), vmem(), vmem()],
        out_specs=vmem(),
        scratch_shapes=[pltpu.VMEM((width // 128, depth * 8, 128), F32)],
        name="enter",
    )(place, occupation.reshape(width * 8, depth), offset.reshape(8, depth), grid_warmth)
    source = lax.all_to_all(code, BOTH, 0, 0, tiled=True)
    low_edge, high_edge = source[:, :8], source[:, rows - 8 :]

    row_warmth = warmth.reshape(1, modes)
    all_courant = lax.all_gather(courant, "mode", axis=1, tiled=True)
    all_quadrant = lax.all_gather(quadrant, "mode", axis=0, tiled=True).reshape(1, modes)
    dims = (slices, ring, lane2, modes, blocks)
    edge = jax.ShapeDtypeStruct((ring, modes), BF16)
    relax = None
    for iteration in range(ITERS):
        first, last = iteration == 0, iteration == ITERS - 1
        low = lax.ppermute(high_edge, BOTH, forward)
        high = lax.ppermute(low_edge, BOTH, backward)
        if last:
            outs = (
                jax.ShapeDtypeStruct((count, rows, width), jnp.int16),
                jax.ShapeDtypeStruct((1, cells + 128), F32),
            )
        else:
            outs = (jax.ShapeDtypeStruct((cells, modes), F32), edge, edge)
            if first:
                outs += (jax.ShapeDtypeStruct((1, modes), F32),)
        operands = [source, low, high, all_courant, all_quadrant, row_warmth, full]
        specs = [vmem()] * 6 + [pl.BlockSpec(memory_space=pl.ANY)]
        if not first:
            operands.append(relax)
            specs.append(vmem())
        scratch = [
            pltpu.VMEM((cells, modes), F32),
            pltpu.VMEM((cells + 16 if first else cells, modes), BF16),
            pltpu.VMEM((blocks, width, modes), BF16),
            pltpu.SemaphoreType.DMA((blocks,)),
        ]
        if first:
            scratch.append(pltpu.VMEM((cells, modes), F32))
        results = pl.pallas_call(
            functools.partial(iterate_kernel, first, last, dims),
            out_shape=outs,
            in_specs=specs,
            out_specs=tuple(vmem() for _ in outs),
            scratch_shapes=scratch,
            compiler_params=pltpu.CompilerParams(vmem_limit_bytes=40 * 2**20),
            name=f"iterate{iteration}",
        )(*operands)
        if last:
            code, aux = results
        else:
            source, low_edge, high_edge = results[:3]
            if first:
                relax = results[3]

    aux_all = lax.all_gather(aux, BOTH, axis=0, tiled=False)
    code = lax.all_to_all(code, BOTH, 0, 0, tiled=True)
    population = pl.pallas_call(
        functools.partial(leave_kernel, order, width, rows, depth),
        out_shape=jax.ShapeDtypeStruct((width * 8, depth), F32),
        in_specs=[vmem(), vmem()],
        out_specs=vmem(),
        scratch_shapes=[pltpu.VMEM((width // 128, depth * 8, 128), F32)],
        name="leave",
    )(code, aux_all)
    thermal = aux_all.reshape(count, -1)[jnp.array(order), :cells]
    thermal = thermal.reshape(count, slices, spaces, planes, lane2)
    thermal = lax.dynamic_index_in_dim(thermal, lax.axis_index("space"), 2, keepdims=False)
    thermal = thermal.transpose(2, 3, 0, 1).reshape(planes, lane2, depth)
    return population.reshape(occupation.shape), thermal


def shards(occupation, offset, warmth, courant, quadrant, matrix):
    count = lax.axis_size("space") * lax.axis_size("mode")
    width, planes, lane2, depth = occupation.shape
    fits = (
        depth % count == 0
        and planes * lane2 == 8
        and 8 % lane2 == 0
        and width % 128 == 0
        and width % (16 * lax.axis_size("space")) == 0
        and (depth // count) % 2 == 0
    )
    form = cell_shards if fits else plain_shards
    return form(occupation, offset, warmth, courant, quadrant, matrix)


def solution(mesh):
    placed = (
        P("mode", "space", None, None),
        P("space", None, None),
        P(),
        P(None, "mode"),
        P("mode"),
        P("mode", None),
    )
    return jax.shard_map(
        shards,
        mesh=mesh,
        in_specs=placed,
        out_specs=(P("mode", "space", None, None), P("space", None, None)),
        check_vma=False,
    )
```

```python
import functools
import jax
import jax.numpy as jnp
from jax import lax
from jax.experimental import pallas as pl
from jax.experimental.pallas import tpu as pltpu
from jax.sharding import PartitionSpec as P

ITERS = 3
BOTH = ("space", "mode")
OCTAVES = 31
STEPS = 1024
F32 = jnp.float32
BF16 = jnp.bfloat16


def padded_2(cells, sides, width):
    for axis, dim in sides:
        count = lax.axis_size(axis)
        head = lax.slice_in_dim(cells, 0, width, axis=dim)
        tail = lax.slice_in_dim(cells, cells.shape[dim] - width, cells.shape[dim], axis=dim)
        cells = jnp.concatenate(
            [
                lax.ppermute(tail, axis, [(i, (i + 1) % count) for i in range(count)]),
                cells,
                lax.ppermute(head, axis, [((i + 1) % count, i) for i in range(count)]),
            ],
            axis=dim,
        )
    return cells


def advect(lattice_wave_carry, courant_numbers, sign_quadrant):
    padded = padded_2(lattice_wave_carry, (("space", 1),), 1)
    advected = lattice_wave_carry
    for dim_index in range(3):
        if dim_index == 0:
            below_side = padded[:, :-2]
            above_side = padded[:, 2:]
        else:
            below_side = jnp.roll(lattice_wave_carry, 1, dim_index + 1)
            above_side = jnp.roll(lattice_wave_carry, -1, dim_index + 1)
        sign_bit = (sign_quadrant >> dim_index & 1).reshape(-1, 1, 1, 1)
        upwind = jnp.where(sign_bit == 1, above_side, below_side)
        advected = advected - courant_numbers[dim_index].reshape(-1, 1, 1, 1) * (
            lattice_wave_carry - upwind
        )
    return advected


def plain_shards(occupation, offset, warmth, courant, quadrant, matrix):
    local_modes = occupation.shape[0]
    extents = occupation.shape
    cell_count = extents[1] * extents[2] * extents[3]
    first_mode = lax.axis_index("mode") * local_modes
    own_warmth = lax.dynamic_slice_in_dim(warmth, first_mode, local_modes)
    total_warmth = jnp.sum(warmth)
    state = occupation + own_warmth.reshape(-1, 1, 1, 1) * offset[None]
    relax = jnp.dot(matrix.astype(F32), warmth, precision=lax.Precision.HIGHEST)
    thermal = jnp.zeros(extents[1:], F32)
    for _ in range(ITERS):
        moved = advect(state, courant, quadrant)
        moved_bf = moved.astype(BF16)
        flat = lax.all_gather(moved_bf, "mode", axis=0, tiled=True).reshape(-1, cell_count)
        product = jnp.dot(matrix, flat, preferred_element_type=F32)
        energy = lax.psum(
            jnp.dot(
                own_warmth,
                moved_bf.reshape(local_modes, cell_count).astype(F32),
                precision=lax.Precision.HIGHEST,
            ),
            "mode",
        )
        thermal = (energy / total_warmth).reshape(extents[1:])
        state = moved - product.reshape(extents) + relax.reshape(-1, 1, 1, 1) * thermal[None]
    return state, thermal


def encode(x, inverse):
    y = jnp.maximum(jnp.abs(x) * inverse, 2.0**-OCTAVES)
    e = jnp.clip(jnp.floor(jnp.log2(y)), -float(OCTAVES), -1.0)
    v = (e + (OCTAVES - 1.0)) + y * jnp.exp2(-e)
    code = (v * STEPS + 0.5).astype(jnp.int32)
    return jnp.where(x < 0, -code, code).astype(jnp.int16)


def decode(code, scale):
    c = code.astype(jnp.int32)
    a = jnp.abs(c)
    e = (a >> 10) - OCTAVES
    f = (a & (STEPS - 1)).astype(F32) * (1.0 / STEPS) + 1.0
    v = f * jnp.exp2(e.astype(F32)) * scale
    return jnp.where(a == 0, 0.0, jnp.where(c < 0, -v, v))


def enter_kernel(order, rows, place, occ, offset, warmth, out, work):
    depth = occ.shape[1]
    modes = occ.shape[0] // 8
    for t in range(modes // 128):
        at = pl.multiple_of(place[1] * modes + t * 128, 128)
        column = jnp.broadcast_to(warmth[:, pl.ds(at, 128)], (depth, 128)).T
        for q in range(8):
            x = occ[pl.ds(t * 1024 + q, 128, stride=8), :]
            x = x + column * offset[pl.ds(q, 1), :]
            work[t, pl.ds(q, depth, stride=8), :] = x.T
        for k, device in enumerate(order):
            out[device, t * rows : (t + 1) * rows, :] = encode(
                work[t, k * rows : (k + 1) * rows, :], 2.0**-5
            )


def leave_kernel(order, rows, slices, growth, code, out, thermal_out, work):
    count = len(order)
    chunks = work.shape[0]
    depth = count * slices
    scales, thermals = [], []
    for device in order:
        note = code[device, chunks * rows : chunks * rows + 8, :].astype(jnp.int32)
        scale = jnp.exp2(note[2:3, :].astype(F32))
        scales.append(scale * growth)
        both = decode(note, scale)
        thermals.append(both[0:1] + both[1:2])
    flat = jnp.concatenate(thermals, axis=0).T
    here = lax.broadcasted_iota(jnp.int32, (count, depth), 0) * slices
    there = lax.broadcasted_iota(jnp.int32, (count, depth), 1)
    thermal = jnp.zeros((8, depth), F32)
    for j in range(slices):
        pick = (here + j == there).astype(F32)
        thermal = thermal + jnp.dot(
            flat[j * 8 : j * 8 + 8], pick, precision=lax.Precision.HIGHEST, preferred_element_type=F32
        )
    thermal_out[...] = thermal
    for t in range(chunks):
        for k, device in enumerate(order):
            work[t, k * rows : (k + 1) * rows, :] = decode(
                code[device, t * rows : (t + 1) * rows, :], scales[k]
            )
        for q in range(8):
            x = work[t, pl.ds(q, depth, stride=8), :]
            out[pl.ds(t * 1024 + q, 128, stride=8), :] = x.T


def collect(place, spaces, blocks, own, parts, full, sems):
    width = own.shape[0]
    part = width // spaces
    s, m = place[0], place[1]
    pltpu.make_async_copy(own, full.at[pl.ds(m * width, width), :], sems.at[m]).start()
    for flip, ref in parts:
        for k in range(1, blocks):
            n = (m + blocks - k) % blocks
            to = n * width + (s ^ flip) * part
            pltpu.make_async_copy(
                ref.at[pl.ds((k - 1) * part, part), :], full.at[pl.ds(to, part), :], sems.at[n]
            ).start()


def iterate_kernel(first, last, dims, *refs):
    slices, ring, lane2, modes, blocks, spaces, flips = dims
    cells = slices * ring
    width = modes // blocks
    rows = slices * 8
    refs = list(refs)
    place, source, low, high, warmth = refs[:5]
    refs = refs[5:]
    if first:
        tables, own = refs[:blocks], refs[blocks]
        parts = list(zip(flips, refs[blocks + 1 : blocks + 1 + len(flips)]))
        refs = refs[blocks + 1 + len(flips) :]
    else:
        table, full, relax_in = refs[:3]
        refs = refs[3:]
    if last:
        code_out = refs[0]
        refs = refs[1:]
    else:
        state_out, low_out, high_out = refs[:3]
        refs = refs[3:]
        if first:
            table, full, relax_out = refs[:3]
            refs = refs[3:]
    moved_ref, left = refs[:2]
    state_ref = source
    if first:
        state_ref, sems = refs[2:]
        collect(place, spaces, blocks, own, parts, full, sems)
        for k in range(blocks):
            n = (place[1] + blocks - k) % blocks
            table[:, pl.ds(pl.multiple_of(n * width, 128), width)] = tables[k][...]
        for s in range(spaces):
            for n in range(blocks):
                for t in range(width // 128):
                    x = decode(source[s * blocks + n, t * rows : (t + 1) * rows, :], 2.0**5)
                    at = slice(n * width + t * 128, n * width + t * 128 + 128)
                    for j in range(slices):
                        state_ref[j * ring + s * 8 : j * ring + s * 8 + 8, at] = x[j * 8 : j * 8 + 8]

    step = 128
    row = lax.broadcasted_iota(jnp.int32, (ring, step), 0) % lane2
    energy = [jnp.zeros((ring, step), F32) for _ in range(slices)]
    largest = jnp.zeros((ring, step), F32)
    capacity = jnp.zeros((1, step), F32)
    for b in range(modes // step):
        at = slice(b * step, (b + 1) * step)
        c = [table[d : d + 1, at] for d in range(3)]
        sign = table[3:4, at].astype(jnp.int32)
        up = [jnp.broadcast_to((sign >> d & 1) == 1, (ring, step)) for d in range(3)]
        w = warmth[:, at]
        capacity = capacity + w
        x = [state_ref[j * ring : (j + 1) * ring, at] for j in range(slices)]
        if first:
            n, t = divmod(b, width // step)
            lo, hi = (
                decode(
                    jnp.concatenate([e[s * blocks + n, t] for s in range(spaces)], axis=0), 2.0**5
                )
                for e in (low, high)
            )
        else:
            lo, hi = low[:, at].astype(F32), high[:, at].astype(F32)
        around = [lo] + x + [hi]
        for j in range(slices):
            y = x[j]
            below, above = pltpu.roll(y, lane2, 0), pltpu.roll(y, ring - lane2, 0)
            u0 = jnp.where(up[0], above, below)
            below = jnp.where(row == 0, pltpu.roll(y, ring - lane2 + 1, 0), pltpu.roll(y, 1, 0))
            above = jnp.where(
                row == lane2 - 1, pltpu.roll(y, lane2 - 1, 0), pltpu.roll(y, ring - 1, 0)
            )
            u1 = jnp.where(up[1], above, below)
            u2 = jnp.where(up[2], around[j + 2], around[j])
            moved = y - c[0] * (y - u0) - c[1] * (y - u1) - c[2] * (y - u2)
            bf = moved.astype(BF16)
            moved_ref[j * ring : (j + 1) * ring, at] = moved
            left[j * ring : (j + 1) * ring, at] = bf
            energy[j] = energy[j] + w * bf.astype(F32)
            if last:
                largest = jnp.maximum(largest, jnp.abs(moved))
    total = jnp.sum(capacity, axis=1, keepdims=True)
    thermal = jnp.concatenate(
        [jnp.sum(e, axis=1, keepdims=True) for e in energy], axis=0
    ) / total

    if first:
        w = warmth[...]
        w_high = w.astype(BF16)
        w_mid = (w - w_high.astype(F32)).astype(BF16)
        w_low = (w - w_high.astype(F32) - w_mid.astype(F32)).astype(BF16)
        pad = jnp.zeros((13, modes), F32)
        left[cells:, :] = jnp.concatenate(
            [w_high.astype(F32), w_mid.astype(F32), w_low.astype(F32), pad], axis=0
        ).astype(BF16)
    if last:
        peak = jnp.max(jnp.max(largest, axis=1, keepdims=True), axis=0, keepdims=True)
        power = jnp.ceil(jnp.log2(jnp.maximum(peak, 2.0**-90))) + 1.0
        inverse = jnp.exp2(-power)
        turned = jnp.concatenate(
            [thermal[j * ring + s * 8 : j * ring + s * 8 + 8] for s in range(spaces) for j in range(slices)],
            axis=0,
        )
        flat = jnp.broadcast_to(turned, (cells, 128)).T[0:8, :]
        coarse = encode(flat, inverse)
        fine = encode(flat - decode(coarse, jnp.exp2(power)), inverse)
        coarse, fine = coarse.astype(jnp.int32), fine.astype(jnp.int32)
        which = lax.broadcasted_iota(jnp.int32, (8, 128), 0)
        pad = jnp.zeros((8, 128 - rows), jnp.int32)
        for s in range(spaces):
            one = jnp.concatenate([coarse[:, s * rows : (s + 1) * rows], pad], axis=1)
            two = jnp.concatenate([fine[:, s * rows : (s + 1) * rows], pad], axis=1)
            note = jnp.where(which == 0, one, jnp.where(which == 1, two, power.astype(jnp.int32)))
            note = note.astype(jnp.int16)
            for n in range(blocks):
                code_out[s * blocks + n, width // 128 * rows :, :] = note
        inverse = inverse * (1.0 / growth_of(modes))

    for n in range(blocks):
        at = slice(n * width, (n + 1) * width)
        block = full.at[pl.ds(n * width, width), :]
        if first:
            pltpu.make_async_copy(block, block, sems.at[n]).wait()
        product = lax.dot_general(
            left[...], block[...], (((1,), (1,)), ((), ())), preferred_element_type=F32
        )
        if first:
            relax = product[cells : cells + 1] + product[cells + 1 : cells + 2]
            relax = relax + product[cells + 2 : cells + 3]
            relax_out[:, at] = relax
        else:
            relax = relax_in[:, at]
        state = moved_ref[:, at] - product[:cells] + relax * thermal
        if last:
            for s in range(spaces):
                for t in range(width // 128):
                    piece = jnp.concatenate(
                        [
                            state[j * ring + s * 8 : j * ring + s * 8 + 8, t * 128 : t * 128 + 128]
                            for j in range(slices)
                        ],
                        axis=0,
                    )
                    code_out[s * blocks + n, t * rows : (t + 1) * rows, :] = encode(piece, inverse)
        else:
            state_out[:, at] = state
            low_out[:, at] = state[:ring].astype(BF16)
            high_out[:, at] = state[cells - ring :].astype(BF16)


def growth_of(modes):
    return 2.0 ** (modes - 1).bit_length() * 4.0


def vmem():
    return pl.BlockSpec(memory_space=pltpu.VMEM)


def ring_order(spaces, blocks):
    pairs = max(spaces // 2, 1)
    walk = [q ^ (q >> 1) for q in range(pairs)] if pairs & (pairs - 1) == 0 else list(range(pairs))
    order = []
    for c, q in enumerate(walk):
        for m in range(blocks) if c % 2 == 0 else reversed(range(blocks)):
            for s in range(q * spaces // pairs, (q + 1) * spaces // pairs):
                order.append(s * blocks + m)
    return order


def gather_parts(matrix, spaces, blocks):
    part = matrix.shape[0] // spaces
    own = lax.dynamic_slice_in_dim(matrix, lax.axis_index("space") * part, part, axis=0)
    turns = [[(i, (i + k) % blocks) for i in range(blocks)] for k in range(1, blocks)]
    arrived = jnp.concatenate([lax.ppermute(own, "mode", turn) for turn in turns], axis=0)

    def flipped(x, flip):
        return lax.ppermute(x, "space", [(s, s ^ flip) for s in range(spaces)])

    parts = {0: arrived}
    for flip in range(2, spaces, 2):
        parts[flip] = flipped(arrived, flip)
    for flip in range(0, spaces, 2):
        parts[flip + 1] = flipped(parts[flip], 1)
    return parts


def cell_shards(occupation, offset, warmth, courant, quadrant, matrix):
    spaces, blocks = lax.axis_size("space"), lax.axis_size("mode")
    width, planes, lane2, depth = occupation.shape
    modes = warmth.shape[0]
    slices = depth // (spaces * blocks)
    ring = spaces * planes * lane2
    cells = slices * ring
    rows = slices * 8
    chunks = width // 128
    order = ring_order(spaces, blocks)
    count = spaces * blocks
    forward = [(order[k], order[(k + 1) % count]) for k in range(count)]
    backward = [(b, a) for a, b in forward]
    place = jnp.stack([lax.axis_index("space"), lax.axis_index("mode")]).astype(jnp.int32)
    row_warmth = warmth.reshape(1, modes)

    parts = gather_parts(matrix, spaces, blocks)
    table = jnp.concatenate([courant, quadrant.astype(F32).reshape(1, width)], axis=0)
    tables = [table] + [
        lax.ppermute(table, "mode", [(i, (i + k) % blocks) for i in range(blocks)])
        for k in range(1, blocks)
    ]

    smem = pl.BlockSpec(memory_space=pltpu.SMEM)
    anywhere = pl.BlockSpec(memory_space=pl.ANY)
    code = pl.pallas_call(
        functools.partial(enter_kernel, order, rows),
        out_shape=jax.ShapeDtypeStruct((count, chunks * rows, 128), jnp.int16),
        in_specs=[smem, vmem(), vmem(), vmem()],
        out_specs=vmem(),
        scratch_shapes=[pltpu.VMEM((chunks, depth * 8, 128), F32)],
        name="enter",
    )(place, occupation.reshape(width * 8, depth), offset.reshape(8, depth), row_warmth)
    code, parts[0] = lax.optimization_barrier((code, parts[0]))
    source = lax.all_to_all(code, BOTH, 0, 0, tiled=True)
    split = source.reshape(count, chunks, rows, 128)
    low_edge, high_edge = split[:, :, :8], split[:, :, rows - 8 :]

    flips = tuple(sorted(parts))
    dims = (slices, ring, lane2, modes, blocks, spaces, flips)
    edge = jax.ShapeDtypeStruct((ring, modes), BF16)
    whole = (
        jax.ShapeDtypeStruct((4, modes), F32),
        jax.ShapeDtypeStruct((modes, modes), BF16),
        jax.ShapeDtypeStruct((1, modes), F32),
    )
    kept = ()
    for iteration in range(ITERS):
        first, last = iteration == 0, iteration == ITERS - 1
        low = lax.ppermute(high_edge, BOTH, forward)
        high = lax.ppermute(low_edge, BOTH, backward)
        if last:
            outs = (jax.ShapeDtypeStruct((count, chunks * rows + 8, 128), jnp.int16),)
        else:
            outs = (jax.ShapeDtypeStruct((cells, modes), F32), edge, edge)
            if first:
                outs += whole
        operands = [place, source, low, high, row_warmth]
        specs = [smem] + [vmem()] * 4
        scratch = [
            pltpu.VMEM((cells, modes), F32),
            pltpu.VMEM((cells + 16 if first else cells, modes), BF16),
        ]
        if first:
            operands += tables + [matrix] + [parts[f] for f in flips]
            specs += [vmem()] * blocks + [anywhere] * (1 + len(flips))
            scratch += [pltpu.VMEM((cells, modes), F32), pltpu.SemaphoreType.DMA((blocks,))]
        else:
            operands += kept
            specs += [vmem()] * 3
        results = pl.pallas_call(
            functools.partial(iterate_kernel, first, last, dims),
            out_shape=outs,
            in_specs=specs,
            out_specs=tuple(vmem() for _ in outs),
            scratch_shapes=scratch,
            compiler_params=pltpu.CompilerParams(vmem_limit_bytes=30 * 2**20),
            name=f"iterate{iteration}",
        )(*operands)
        if last:
            code = results[0]
        else:
            source, low_edge, high_edge = results[:3]
            kept = kept or results[3:]

    code = lax.all_to_all(code, BOTH, 0, 0, tiled=True)
    population, thermal = pl.pallas_call(
        functools.partial(leave_kernel, order, rows, slices, growth_of(modes)),
        out_shape=(
            jax.ShapeDtypeStruct((width * 8, depth), F32),
            jax.ShapeDtypeStruct((8, depth), F32),
        ),
        in_specs=[vmem()],
        out_specs=(vmem(), vmem()),
        scratch_shapes=[pltpu.VMEM((chunks, depth * 8, 128), F32)],
        name="leave",
    )(code)
    return population.reshape(occupation.shape), thermal.reshape(offset.shape)


def shards(occupation, offset, warmth, courant, quadrant, matrix):
    count = lax.axis_size("space") * lax.axis_size("mode")
    width, planes, lane2, depth = occupation.shape
    fits = (
        depth == 128
        and depth % count == 0
        and lax.axis_size("space") & (lax.axis_size("space") - 1) == 0
        and lax.axis_size("space") > 1
        and planes * lane2 == 8
        and 8 % lane2 == 0
        and width % 128 == 0
        and width % (16 * lax.axis_size("space")) == 0
        and (depth // count) % 2 == 0
    )
    form = cell_shards if fits else plain_shards
    return form(occupation, offset, warmth, courant, quadrant, matrix)


def solution(mesh):
    placed = (
        P("mode", "space", None, None),
        P("space", None, None),
        P(),
        P(None, "mode"),
        P("mode"),
        P("mode", None),
    )
    return jax.shard_map(
        shards,
        mesh=mesh,
        in_specs=placed,
        out_specs=(P("mode", "space", None, None), P("space", None, None)),
        check_vma=False,
    )
```

```python
import functools
import jax
import jax.numpy as jnp
from jax import lax
from jax.experimental import pallas as pl
from jax.experimental.pallas import tpu as pltpu
from jax.sharding import PartitionSpec as P

ITERS = 3
BOTH = ("space", "mode")
OCTAVES = 31
STEPS = 1024
F32 = jnp.float32
BF16 = jnp.bfloat16


def padded_2(cells, sides, width):
    for axis, dim in sides:
        count = lax.axis_size(axis)
        head = lax.slice_in_dim(cells, 0, width, axis=dim)
        tail = lax.slice_in_dim(cells, cells.shape[dim] - width, cells.shape[dim], axis=dim)
        cells = jnp.concatenate(
            [
                lax.ppermute(tail, axis, [(i, (i + 1) % count) for i in range(count)]),
                cells,
                lax.ppermute(head, axis, [((i + 1) % count, i) for i in range(count)]),
            ],
            axis=dim,
        )
    return cells


def advect(lattice_wave_carry, courant_numbers, sign_quadrant):
    padded = padded_2(lattice_wave_carry, (("space", 1),), 1)
    advected = lattice_wave_carry
    for dim_index in range(3):
        if dim_index == 0:
            below_side = padded[:, :-2]
            above_side = padded[:, 2:]
        else:
            below_side = jnp.roll(lattice_wave_carry, 1, dim_index + 1)
            above_side = jnp.roll(lattice_wave_carry, -1, dim_index + 1)
        sign_bit = (sign_quadrant >> dim_index & 1).reshape(-1, 1, 1, 1)
        upwind = jnp.where(sign_bit == 1, above_side, below_side)
        advected = advected - courant_numbers[dim_index].reshape(-1, 1, 1, 1) * (
            lattice_wave_carry - upwind
        )
    return advected


def plain_shards(occupation, offset, warmth, courant, quadrant, matrix):
    local_modes = occupation.shape[0]
    extents = occupation.shape
    cell_count = extents[1] * extents[2] * extents[3]
    first_mode = lax.axis_index("mode") * local_modes
    own_warmth = lax.dynamic_slice_in_dim(warmth, first_mode, local_modes)
    total_warmth = jnp.sum(warmth)
    state = occupation + own_warmth.reshape(-1, 1, 1, 1) * offset[None]
    relax = jnp.dot(matrix.astype(F32), warmth, precision=lax.Precision.HIGHEST)
    thermal = jnp.zeros(extents[1:], F32)
    for _ in range(ITERS):
        moved = advect(state, courant, quadrant)
        moved_bf = moved.astype(BF16)
        flat = lax.all_gather(moved_bf, "mode", axis=0, tiled=True).reshape(-1, cell_count)
        product = jnp.dot(matrix, flat, preferred_element_type=F32)
        energy = lax.psum(
            jnp.dot(
                own_warmth,
                moved_bf.reshape(local_modes, cell_count).astype(F32),
                precision=lax.Precision.HIGHEST,
            ),
            "mode",
        )
        thermal = (energy / total_warmth).reshape(extents[1:])
        state = moved - product.reshape(extents) + relax.reshape(-1, 1, 1, 1) * thermal[None]
    return state, thermal


def encode(x, inverse):
    y = jnp.maximum(jnp.abs(x) * inverse, 2.0**-OCTAVES)
    e = jnp.clip(jnp.floor(jnp.log2(y)), -float(OCTAVES), -1.0)
    v = (e + (OCTAVES - 1.0)) + y * jnp.exp2(-e)
    code = (v * STEPS + 0.5).astype(jnp.int32)
    return jnp.where(x < 0, -code, code).astype(jnp.int16)


def decode(code, scale):
    c = code.astype(jnp.int32)
    a = jnp.abs(c)
    e = (a >> 10) - OCTAVES
    f = (a & (STEPS - 1)).astype(F32) * (1.0 / STEPS) + 1.0
    v = f * jnp.exp2(e.astype(F32)) * scale
    return jnp.where(a == 0, 0.0, jnp.where(c < 0, -v, v))


def enter_kernel(order, rows, place, occ, offset, warmth, out, work):
    depth = occ.shape[1]
    modes = occ.shape[0] // 8
    for t in range(modes // 128):
        at = pl.multiple_of(place[1] * modes + t * 128, 128)
        column = jnp.broadcast_to(warmth[:, pl.ds(at, 128)], (depth, 128)).T
        for q in range(8):
            x = occ[pl.ds(t * 1024 + q, 128, stride=8), :]
            x = x + column * offset[pl.ds(q, 1), :]
            work[t, pl.ds(q, depth, stride=8), :] = x.T
        for k, device in enumerate(order):
            out[device, t * rows : (t + 1) * rows, :] = encode(
                work[t, k * rows : (k + 1) * rows, :], 2.0**-5
            )


def leave_kernel(order, rows, slices, growth, code, out, thermal_out, work):
    count = len(order)
    chunks = work.shape[0]
    depth = count * slices
    scales, thermals = [], []
    for device in order:
        note = code[device, chunks * rows : chunks * rows + 8, :].astype(jnp.int32)
        scale = jnp.exp2(note[2:3, :].astype(F32))
        scales.append(scale * growth)
        both = decode(note, scale)
        thermals.append(both[0:1] + both[1:2])
    flat = jnp.concatenate(thermals, axis=0).T
    here = lax.broadcasted_iota(jnp.int32, (count, depth), 0) * slices
    there = lax.broadcasted_iota(jnp.int32, (count, depth), 1)
    thermal = jnp.zeros((8, depth), F32)
    for j in range(slices):
        pick = (here + j == there).astype(F32)
        thermal = thermal + jnp.dot(
            flat[j * 8 : j * 8 + 8], pick, precision=lax.Precision.HIGHEST, preferred_element_type=F32
        )
    thermal_out[...] = thermal
    for t in range(chunks):
        for k, device in enumerate(order):
            work[t, k * rows : (k + 1) * rows, :] = decode(
                code[device, t * rows : (t + 1) * rows, :], scales[k]
            )
        for q in range(8):
            x = work[t, pl.ds(q, depth, stride=8), :]
            out[pl.ds(t * 1024 + q, 128, stride=8), :] = x.T


def collect(place, spaces, blocks, own, parts, full, sems):
    width = own.shape[0]
    part = width // spaces
    s, m = place[0], place[1]
    pltpu.make_async_copy(own, full.at[pl.ds(m * width, width), :], sems.at[m]).start()
    for (k, flip), ref in parts:
        n = (m + blocks - k) % blocks
        to = n * width + (s ^ flip) * part
        pltpu.make_async_copy(ref, full.at[pl.ds(to, part), :], sems.at[n]).start()


def widen(x, width):
    return jnp.broadcast_to(x, (x.shape[0], width))


def decode_kernel(dims, source, state_ref):
    slices, ring, _, modes, blocks, spaces, _ = dims
    width = modes // blocks
    rows = slices * 8
    for s in range(spaces):
        for n in range(blocks):
            for t in range(width // 128):
                x = decode(source[s * blocks + n, t * rows : (t + 1) * rows, :], 2.0**5)
                at = slice(n * width + t * 128, n * width + t * 128 + 128)
                for j in range(slices):
                    state_ref[j * ring + s * 8 : j * ring + s * 8 + 8, at] = x[j * 8 : j * 8 + 8]


def move(first, last, dims, place, state_ref, low, high, warmth, table, moved_ref, left, tables):
    slices, ring, lane2, modes, blocks, spaces, _ = dims
    cells = slices * ring
    width = modes // blocks
    if first:
        for k in range(blocks):
            n = (place[1] + blocks - k) % blocks
            table[:, pl.ds(pl.multiple_of(n * width, 128), width)] = tables[k][...]
    step = 128
    row = lax.broadcasted_iota(jnp.int32, (ring, step), 0) % lane2
    energy = [jnp.zeros((ring, step), F32) for _ in range(slices)]
    largest = jnp.zeros((ring, step), F32)
    capacity = jnp.zeros((1, step), F32)
    for b in range(modes // step):
        at = slice(b * step, (b + 1) * step)
        c = [table[d : d + 1, at] for d in range(3)]
        sign = table[3:4, at].astype(jnp.int32)
        up = [jnp.broadcast_to((sign >> d & 1) == 1, (ring, step)) for d in range(3)]
        w = warmth[:, at]
        capacity = capacity + w
        x = [state_ref[j * ring : (j + 1) * ring, at] for j in range(slices)]
        if first:
            n, t = divmod(b, width // step)
            lo, hi = (
                decode(
                    jnp.concatenate([e[s * blocks + n, t] for s in range(spaces)], axis=0), 2.0**5
                )
                for e in (low, high)
            )
        else:
            lo, hi = low[:, at].astype(F32), high[:, at].astype(F32)
        around = [lo] + x + [hi]
        for j in range(slices):
            y = x[j]
            below, above = pltpu.roll(y, lane2, 0), pltpu.roll(y, ring - lane2, 0)
            u0 = jnp.where(up[0], above, below)
            below = jnp.where(row == 0, pltpu.roll(y, ring - lane2 + 1, 0), pltpu.roll(y, 1, 0))
            above = jnp.where(
                row == lane2 - 1, pltpu.roll(y, lane2 - 1, 0), pltpu.roll(y, ring - 1, 0)
            )
            u1 = jnp.where(up[1], above, below)
            u2 = jnp.where(up[2], around[j + 2], around[j])
            moved = y - c[0] * (y - u0) - c[1] * (y - u1) - c[2] * (y - u2)
            bf = moved.astype(BF16)
            moved_ref[j * ring : (j + 1) * ring, at] = moved
            left[j * ring : (j + 1) * ring, at] = bf
            energy[j] = energy[j] + w * bf.astype(F32)
            if last:
                largest = jnp.maximum(largest, jnp.abs(moved))
    total = jnp.sum(capacity, axis=1, keepdims=True)
    thermal = jnp.concatenate(
        [jnp.sum(e, axis=1, keepdims=True) for e in energy], axis=0
    ) / total

    if first:
        w = warmth[...]
        w_high = w.astype(BF16)
        w_mid = (w - w_high.astype(F32)).astype(BF16)
        w_low = (w - w_high.astype(F32) - w_mid.astype(F32)).astype(BF16)
        pad = jnp.zeros((13, modes), F32)
        left[cells:, :] = jnp.concatenate(
            [w_high.astype(F32), w_mid.astype(F32), w_low.astype(F32), pad], axis=0
        ).astype(BF16)
    peak = jnp.max(jnp.max(largest, axis=1, keepdims=True), axis=0, keepdims=True)
    return thermal, peak


def iterate_kernel(first, last, stage, dims, *refs):
    slices, ring, _, modes, blocks, spaces, keys = dims
    cells = slices * ring
    width = modes // blocks
    rows = slices * 8
    refs = list(refs)
    if stage == "apply":
        place, moved_ref, left, heat, own = refs[:5]
        parts = list(zip(keys, refs[5 : 5 + len(keys)]))
        state_out, low_out, high_out, full, relax_out, sems = refs[5 + len(keys) :]
        collect(place, spaces, blocks, own, parts, full, sems)
        thermal = heat[:, 0:1]
    else:
        place, state_ref, low, high, warmth = refs[:5]
        refs = refs[5:]
        if first:
            tables, refs = refs[:blocks], refs[blocks:]
            moved_ref, left, heat, table = refs
        else:
            table, full, relax_in = refs[:3]
            refs = refs[3:]
            if last:
                code_out, moved_ref, left = refs
            else:
                state_out, low_out, high_out, moved_ref, left = refs
        thermal, peak = move(
            first, last, dims, place, state_ref, low, high, warmth, table, moved_ref, left,
            tables if first else None,
        )
        if first:
            heat[...] = widen(thermal, 128)
            return
    if last:
        power = jnp.ceil(jnp.log2(jnp.maximum(peak, 2.0**-90))) + 1.0
        inverse = jnp.exp2(-power)
        turned = jnp.concatenate(
            [thermal[j * ring + s * 8 : j * ring + s * 8 + 8] for s in range(spaces) for j in range(slices)],
            axis=0,
        )
        flat = jnp.broadcast_to(turned, (cells, 128)).T[0:8, :]
        coarse = encode(flat, inverse)
        fine = encode(flat - decode(coarse, jnp.exp2(power)), inverse)
        coarse, fine = coarse.astype(jnp.int32), fine.astype(jnp.int32)
        which = lax.broadcasted_iota(jnp.int32, (8, 128), 0)
        pad = jnp.zeros((8, 128 - rows), jnp.int32)
        for s in range(spaces):
            one = jnp.concatenate([coarse[:, s * rows : (s + 1) * rows], pad], axis=1)
            two = jnp.concatenate([fine[:, s * rows : (s + 1) * rows], pad], axis=1)
            note = jnp.where(which == 0, one, jnp.where(which == 1, two, power.astype(jnp.int32)))
            note = note.astype(jnp.int16)
            for n in range(blocks):
                code_out[s * blocks + n, width // 128 * rows :, :] = note
        inverse = inverse * (1.0 / growth_of(modes))

    for n in range(blocks):
        at = slice(n * width, (n + 1) * width)
        block = full.at[pl.ds(n * width, width), :]
        if first:
            pltpu.make_async_copy(block, block, sems.at[n]).wait()
        product = lax.dot_general(
            left[...], block[...], (((1,), (1,)), ((), ())), preferred_element_type=F32
        )
        if first:
            relax = product[cells : cells + 1] + product[cells + 1 : cells + 2]
            relax = relax + product[cells + 2 : cells + 3]
            relax_out[:, at] = relax
        else:
            relax = relax_in[:, at]
        state = moved_ref[:, at] - product[:cells] + relax * thermal
        if last:
            for s in range(spaces):
                for t in range(width // 128):
                    piece = jnp.concatenate(
                        [
                            state[j * ring + s * 8 : j * ring + s * 8 + 8, t * 128 : t * 128 + 128]
                            for j in range(slices)
                        ],
                        axis=0,
                    )
                    code_out[s * blocks + n, t * rows : (t + 1) * rows, :] = encode(piece, inverse)
        else:
            state_out[:, at] = state
            low_out[:, at] = state[:ring].astype(BF16)
            high_out[:, at] = state[cells - ring :].astype(BF16)


def growth_of(modes):
    return 2.0 ** (modes - 1).bit_length() * 4.0


def vmem():
    return pl.BlockSpec(memory_space=pltpu.VMEM)


def ring_order(spaces, blocks):
    pairs = max(spaces // 2, 1)
    walk = [q ^ (q >> 1) for q in range(pairs)] if pairs & (pairs - 1) == 0 else list(range(pairs))
    order = []
    for c, q in enumerate(walk):
        for m in range(blocks) if c % 2 == 0 else reversed(range(blocks)):
            for s in range(q * spaces // pairs, (q + 1) * spaces // pairs):
                order.append(s * blocks + m)
    return order


def gather_parts(matrix, spaces, blocks):
    part = matrix.shape[0] // spaces
    own = lax.dynamic_slice_in_dim(matrix, lax.axis_index("space") * part, part, axis=0)

    def flipped(x, flip):
        return lax.ppermute(x, "space", [(s, s ^ flip) for s in range(spaces)])

    parts = {}
    for k in range(1, blocks):
        parts[k, 0] = lax.ppermute(own, "mode", [(i, (i + k) % blocks) for i in range(blocks)])
    for k in range(1, blocks):
        for flip in range(2, spaces, 2):
            parts[k, flip] = flipped(parts[k, 0], flip)
        for flip in range(0, spaces, 2):
            parts[k, flip + 1] = flipped(parts[k, flip], 1)
    return parts


def cell_shards(occupation, offset, warmth, courant, quadrant, matrix):
    spaces, blocks = lax.axis_size("space"), lax.axis_size("mode")
    width, planes, lane2, depth = occupation.shape
    modes = warmth.shape[0]
    slices = depth // (spaces * blocks)
    ring = spaces * planes * lane2
    cells = slices * ring
    rows = slices * 8
    chunks = width // 128
    order = ring_order(spaces, blocks)
    count = spaces * blocks
    forward = [(order[k], order[(k + 1) % count]) for k in range(count)]
    backward = [(b, a) for a, b in forward]
    place = jnp.stack([lax.axis_index("space"), lax.axis_index("mode")]).astype(jnp.int32)
    row_warmth = warmth.reshape(1, modes)

    parts = gather_parts(matrix, spaces, blocks)
    table = jnp.concatenate([courant, quadrant.astype(F32).reshape(1, width)], axis=0)
    tables = [table]
    for k in range(1, blocks):
        tables.append(lax.ppermute(table, "mode", [(i, (i + k) % blocks) for i in range(blocks)]))

    smem = pl.BlockSpec(memory_space=pltpu.SMEM)
    anywhere = pl.BlockSpec(memory_space=pl.ANY)
    code = pl.pallas_call(
        functools.partial(enter_kernel, order, rows),
        out_shape=jax.ShapeDtypeStruct((count, chunks * rows, 128), jnp.int16),
        in_specs=[smem, vmem(), vmem(), vmem()],
        out_specs=vmem(),
        scratch_shapes=[pltpu.VMEM((chunks, depth * 8, 128), F32)],
        compiler_params=pltpu.CompilerParams(vmem_limit_bytes=12 * 2**20),
        name="enter",
    )(place, occupation.reshape(width * 8, depth), offset.reshape(8, depth), row_warmth)
    source = lax.all_to_all(code, BOTH, 0, 0, tiled=True)
    split = source.reshape(count, chunks, rows, 128)
    low_edge, high_edge = split[:, :, :8], split[:, :, rows - 8 :]

    keys = tuple(sorted(parts))
    dims = (slices, ring, lane2, modes, blocks, spaces, keys)
    state = jax.ShapeDtypeStruct((cells, modes), F32)
    edge = jax.ShapeDtypeStruct((ring, modes), BF16)
    left = jax.ShapeDtypeStruct((cells + 16, modes), BF16)
    row = jax.ShapeDtypeStruct((1, modes), F32)
    scratch = [pltpu.VMEM((cells, modes), F32), pltpu.VMEM((cells, modes), BF16)]

    def call(first, last, stage, outs, specs, scratch, operands):
        return pl.pallas_call(
            functools.partial(iterate_kernel, first, last, stage, dims),
            out_shape=outs,
            in_specs=specs,
            out_specs=tuple(vmem() for _ in outs),
            scratch_shapes=scratch,
            compiler_params=pltpu.CompilerParams(vmem_limit_bytes=22 * 2**20),
        )(*operands)

    source = pl.pallas_call(
        functools.partial(decode_kernel, dims),
        out_shape=state,
        in_specs=[vmem()],
        out_specs=vmem(),
        compiler_params=pltpu.CompilerParams(vmem_limit_bytes=8 * 2**20),
        name="decode",
    )(source)
    for iteration in range(ITERS):
        first, last = iteration == 0, iteration == ITERS - 1
        low = lax.ppermute(high_edge, BOTH, forward)
        high = lax.ppermute(low_edge, BOTH, backward)
        operands = [place, source, low, high, row_warmth]
        specs = [smem] + [vmem()] * 4
        if first:
            moved, bf, heat, table = call(
                True, False, "move",
                (state, left, jax.ShapeDtypeStruct((cells, 128), F32), jax.ShapeDtypeStruct((4, modes), F32)),
                specs + [vmem()] * blocks,
                [],
                operands + tables,
            )
            source, low_edge, high_edge, full, relax = call(
                True, False, "apply",
                (state, edge, edge, jax.ShapeDtypeStruct((modes, modes), BF16), row),
                [smem] + [vmem()] * 3 + [anywhere] * (1 + len(keys)),
                [pltpu.SemaphoreType.DMA((blocks,))],
                [place, moved, bf, heat, matrix] + [parts[key] for key in keys],
            )
            continue
        operands += [table, full, relax]
        specs += [vmem()] * 3
        if last:
            outs = (jax.ShapeDtypeStruct((count, chunks * rows + 8, 128), jnp.int16),)
        else:
            outs = (state, edge, edge)
        results = call(False, last, None, outs, specs, scratch, operands)
        if last:
            code = results[0]
        else:
            source, low_edge, high_edge = results

    code = lax.all_to_all(code, BOTH, 0, 0, tiled=True)
    population, thermal = pl.pallas_call(
        functools.partial(leave_kernel, order, rows, slices, growth_of(modes)),
        out_shape=(
            jax.ShapeDtypeStruct((width * 8, depth), F32),
            jax.ShapeDtypeStruct((8, depth), F32),
        ),
        in_specs=[vmem()],
        out_specs=(vmem(), vmem()),
        scratch_shapes=[pltpu.VMEM((chunks, depth * 8, 128), F32)],
        compiler_params=pltpu.CompilerParams(vmem_limit_bytes=12 * 2**20),
        name="leave",
    )(code)
    return population.reshape(occupation.shape), thermal.reshape(offset.shape)


def fits(spaces, blocks, width, planes, lane2, depth):
    count = spaces * blocks
    return (
        depth == 128
        and depth % count == 0
        and (depth // count) % 2 == 0
        and spaces > 1
        and spaces & (spaces - 1) == 0
        and planes * lane2 == 8
        and width % 128 == 0
        and width % (16 * spaces) == 0
    )


def shards(occupation, offset, warmth, courant, quadrant, matrix):
    arguments = (occupation, offset, warmth, courant, quadrant, matrix)
    if fits(lax.axis_size("space"), lax.axis_size("mode"), *occupation.shape):
        return cell_shards(*arguments)
    return plain_shards(*arguments)


def solution(mesh):
    placed = (
        P("mode", "space", None, None),
        P("space", None, None),
        P(),
        P(None, "mode"),
        P("mode"),
        P("mode", None),
    )
    return jax.shard_map(
        shards,
        mesh=mesh,
        in_specs=placed,
        out_specs=(P("mode", "space", None, None), P("space", None, None)),
        check_vma=False,
    )
```
